32 devices in a mesh: dev: 16 (over z, y, x), rep: 2 (over core).
Axes of the slice: x: 2, y: 2, z: 4, core: 2. Of those that a mesh axis runs over, the one named last changes fastest.
Arguments:
- node_features: bfloat16 [1024, 2, 3136], P('dev', 'rep'), may hold values from -6 to 6
- src_node: int32 [16, 16, 2], P('dev'), may hold values from 0 to 63
- dst_node: int32 [16, 16, 2], P('dev'), may hold values from 0 to 63
- counts: int32 [16, 16], P('dev'), may hold values from 1 to 2, as said below
- rotation: bfloat16 [16, 16, 2, 235], P('dev'), may hold values from -2 to 2
- w_zero: bfloat16 [896, 2, 448], P(None, 'rep'), may hold values from -0.1875 to 0.1875
- w_one: bfloat16 [2, 768, 2, 384], P(None, None, 'rep'), may hold values from -0.15625 to 0.15625
- w_two: bfloat16 [2, 640, 2, 320], P(None, None, 'rep'), may hold values from -0.15625 to 0.15625
- norm_gain: float32 [2, 3136], P('rep'), may hold values from 0.5 to 1.5
Outputs:
- updated: bfloat16 [1024, 2, 3136], P('dev', 'rep')
The draws below stay inside these ranges and needn't reach their ends.
Inputs may be any that keep to these rules, and one draw needn't show every extreme that they name: Slots i < counts[s, d] hold edges, the others padding; in every draw some destination device receives 2 edges from every source device.
All inputs are finite; a program needn't handle non-finite values.
Results may differ from the reference program's by a relative error of at most 0.0054.
Values may be sent and summed in bfloat16 or wider, within the bound.
A program may use at most 64 MiB of HBM per device.

```python
import jax
import jax.numpy as jnp
from jax import lax

C = 128
COEFFS = 49
ROT = 235
NODE_DEV = 64
CAP = 2
CH = 64
NODES = 1024
N_DEV = 16
N_REP = 2


def draw_counts(key, part):
    counts_base = jax.random.randint(jax.random.fold_in(key, 11), (N_DEV, N_DEV), 1, CAP + 1)
    hot_dest = jax.random.randint(jax.random.fold_in(key, 12), (2,), 0, N_DEV)
    column = jnp.arange(N_DEV)
    is_hot = (column[None, :] == hot_dest[0]) | (column[None, :] == hot_dest[1])
    return jnp.where(is_hot, CAP, counts_base).astype(jnp.int32)


def touch_ends(values, key, least, largest):
    longest = values.shape.index(max(values.shape))
    spots = []
    for shift in (0, 1):
        where = [jax.random.randint(jax.random.fold_in(key, axis), (), 0, length) for axis, length in enumerate(values.shape)]
        where[longest] = (where[longest] + shift) % values.shape[longest]
        spots.append(tuple(where))
    return values.at[spots[0]].set(least).at[spots[1]].set(largest)


def block_levels(rng, shape, cuts, least, largest):
    def one(dim, blocks):
        heights = jax.random.uniform(jax.random.fold_in(jax.random.fold_in(rng, 6), dim), (blocks,), jnp.float32, least / len(cuts), largest / len(cuts))
        return jnp.repeat(jnp.exp(heights), shape[dim] // blocks).reshape((-1,) + (1,) * (len(shape) - dim - 1))

    gain = one(*cuts[0])
    for cut in cuts[1:]:
        gain = gain * one(*cut)
    return gain


def centred(own_key, shape, spread, most, cuts=(), dtype=jnp.bfloat16):
    values = spread * jax.random.normal(own_key, shape, jnp.float32)
    if cuts:
        values = values * block_levels(own_key, shape, cuts, -0.22, 0.18)
    return jnp.clip(values, -most, most).astype(dtype)


def setup_inputs(seed: int = 0) -> dict:
    key_list = jax.random.split(jax.random.key(seed), 10)
    return {
        "node_features": centred(key_list[0], (NODES, N_REP, COEFFS * CH), 1.0, 6.0, ((0, 16), (1, 2))),
        "src_node": touch_ends(jax.random.randint(key_list[1], (N_DEV, N_DEV, CAP), 0, NODE_DEV), jax.random.fold_in(key_list[1], 1), 0, NODE_DEV - 1).astype(jnp.int32),
        "dst_node": touch_ends(jax.random.randint(key_list[2], (N_DEV, N_DEV, CAP), 0, NODE_DEV), jax.random.fold_in(key_list[2], 1), 0, NODE_DEV - 1).astype(jnp.int32),
        "counts": draw_counts(jax.random.fold_in(key_list[9], 71), 0),
        "rotation": centred(key_list[4], (N_DEV, N_DEV, CAP, ROT), 0.35, 2.0, ((0, 16),)),
        "w_zero": centred(key_list[5], (7 * C, N_REP, 7 * CH), (7 * C) ** -0.5, 0.1875, ((1, 2),)),
        "w_one": centred(key_list[6], (2, 6 * C, N_REP, 6 * CH), (12 * C) ** -0.5, 0.15625, ((2, 2),)),
        "w_two": centred(key_list[7], (2, 5 * C, N_REP, 5 * CH), (10 * C) ** -0.5, 0.15625, ((2, 2),)),
        "norm_gain": jnp.clip(1.0 + 0.1 * jax.random.normal(key_list[8], (N_REP, COEFFS * CH), jnp.float32), 0.5, 1.5),
    }


def frame_slot(degree, order):
    if order == 0:
        return degree
    if order == 1:
        return 6 + degree
    if order == -1:
        return 12 + degree
    if order == 2:
        return 17 + degree
    return 22 + degree

def frame_tables():
    offsets = []
    places = []
    spot = 0
    for degree in range(7):
        reach = min(degree, 2)
        offsets.append(spot)
        spot += (2 * degree + 1) * (2 * reach + 1)
        places.append([frame_slot(degree, order) for order in range(-reach, reach + 1)])
    return (offsets, places)

def rounded(value):
    return lax.optimization_barrier(value.astype(jnp.bfloat16)).astype(jnp.float32)

def block_of(rotation, offsets, degree):
    reach = min(degree, 2)
    span = 2 * degree + 1
    height = 2 * reach + 1
    piece = rotation[:, offsets[degree]:offsets[degree] + height * span]
    return piece.reshape(rotation.shape[0], height, span).astype(jnp.float32)

def frame(coeffs, rotation):
    offsets, places = frame_tables()
    pieces = []
    for degree in range(7):
        matrix = block_of(rotation, offsets, degree)
        part = coeffs[:, degree * degree:degree * degree + 2 * degree + 1, :].astype(jnp.float32)
        pieces.append(lax.optimization_barrier(jnp.sum(matrix[:, :, :, None] * part[:, None, :, :], axis=2)))
    listing = sorted(((places[degree][row], degree, row) for degree in range(7) for row in range(len(places[degree]))))
    return jnp.concatenate([pieces[degree][:, row:row + 1, :] for place, degree, row in listing], axis=1)

def unframe(framed, rotation):
    offsets, places = frame_tables()
    parts = []
    for degree in range(7):
        matrix = block_of(rotation, offsets, degree)
        chosen = jnp.concatenate([framed[:, place:place + 1, :] for place in places[degree]], axis=1).astype(jnp.float32)
        parts.append(lax.optimization_barrier(jnp.sum(matrix[:, :, :, None] * chosen[:, :, None, :], axis=1)))
    return jnp.concatenate(parts, axis=1)

def mix_orders(rotated, zero_mat, one_mats, two_mats):
    batch = rotated.shape[0]
    out_width = zero_mat.shape[1] // 7
    flat_zero = rotated[:, 0:7, :].reshape(batch, -1)
    result = [jnp.dot(flat_zero, zero_mat, preferred_element_type=jnp.float32).reshape(batch, 7, out_width)]
    for first, count, mats in ((7, 6, one_mats), (19, 5, two_mats)):
        plus = rotated[:, first:first + count, :].reshape(batch, -1)
        minus = rotated[:, first + count:first + 2 * count, :].reshape(batch, -1)
        upper = jnp.dot(plus, mats[0], preferred_element_type=jnp.float32) - jnp.dot(minus, mats[1], preferred_element_type=jnp.float32)
        lower = jnp.dot(plus, mats[1], preferred_element_type=jnp.float32) + jnp.dot(minus, mats[0], preferred_element_type=jnp.float32)
        result.append(upper.reshape(batch, count, out_width))
        result.append(lower.reshape(batch, count, out_width))
    return jnp.concatenate(result, axis=1)

def reference(node_features, src_node, dst_node, counts, rotation, w_zero, w_one, w_two, norm_gain):
    nodes, halves, flat = node_features.shape
    half_width = flat // 49
    width = halves * half_width
    full = node_features.reshape(nodes, halves, 49, half_width).transpose(0, 2, 1, 3).reshape(nodes, 49, width)
    zero_mat = w_zero.reshape(7 * width, halves, 7, half_width).transpose(0, 2, 1, 3).reshape(7 * width, 7 * width)
    one_mats = w_one.reshape(2, 6 * width, halves, 6, half_width).transpose(0, 1, 3, 2, 4).reshape(2, 6 * width, 6 * width)
    two_mats = w_two.reshape(2, 5 * width, halves, 5, half_width).transpose(0, 1, 3, 2, 4).reshape(2, 5 * width, 5 * width)
    slots = jnp.arange(CAP).astype(jnp.int32)
    owners = jnp.arange(N_DEV).astype(jnp.int32)

    def one_source(total, source):
        sources = (source * NODE_DEV + src_node[source].reshape(-1)).astype(jnp.int32)
        gathered = jnp.take(full, sources, axis=0)
        rot_rows = rotation[source].reshape(-1, 235)
        rotated = rounded(frame(gathered, rot_rows)).astype(jnp.bfloat16)
        edge_out = rounded(mix_orders(rotated, zero_mat, one_mats, two_mats))
        back = rounded(unframe(edge_out, rot_rows))
        live = (slots[None, :] < counts[source][:, None]).reshape(-1).astype(jnp.float32)
        back = back * live[:, None, None]
        targets = (owners[:, None] * NODE_DEV + dst_node[:, source, :]).reshape(-1).astype(jnp.int32)
        return (total.at[targets].add(back), None)
    total, unused = lax.scan(one_source, jnp.zeros((nodes, 49, width), jnp.float32), owners)
    mean_sq = lax.optimization_barrier(jnp.sum(total * total, axis=(1, 2))) / (49 * width)
    normed = total * lax.rsqrt(mean_sq + 1e-06)[:, None, None]
    normed = normed.reshape(nodes, 49, halves, half_width).transpose(0, 2, 1, 3).reshape(nodes, halves, flat)
    updated = node_features.astype(jnp.float32) + norm_gain[None].astype(jnp.float32) * normed
    return updated.astype(jnp.bfloat16)
```

```python
import functools

import jax
import jax.numpy as jnp
from jax import lax
from jax.experimental import pallas as pl
from jax.experimental.pallas import tpu as pltpu
from jax.sharding import PartitionSpec as P

LANES = 128
HALF = 64
COEFFS = 49
FRAME = 29
ROT = 235
WINDOW = 120
TILES = (COEFFS + 1) // 2
WIDE = TILES * LANES
GROUPS = ((0, 7, 0), (7, 6, 512), (13, 6, 896), (19, 5, 1280), (24, 5, 1664))
MESSAGE = 2048
BLOCK = 32
MESH = pl.DeviceIdType.MESH


def frame_slot(degree, order):
    if order == 0:
        return degree
    if order == 1:
        return 6 + degree
    if order == -1:
        return 12 + degree
    if order == 2:
        return 17 + degree
    return 22 + degree


def terms():
    listing = []
    spot = 0
    for degree in range(7):
        reach = min(degree, 2)
        span = 2 * degree + 1
        first = degree * degree
        for row in range(2 * reach + 1):
            slot = frame_slot(degree, row - reach)
            for tile in range(first // 2, (first + span - 1) // 2 + 1):
                ends = []
                for coeff in (2 * tile, 2 * tile + 1):
                    inside = first <= coeff < first + span
                    ends.append(spot + row * span + coeff - first if inside else None)
                listing.append((slot, tile, ends[0], ends[1]))
        spot += span * (2 * reach + 1)
    return listing


TERMS = terms()


def message_place(slot):
    for first, count, base in GROUPS:
        if first <= slot < first + count:
            lane = base + (slot - first) * HALF
            return lane // LANES, (lane % LANES) // HALF
    raise ValueError


def each(count, func):
    if count <= 16:
        for index in range(count):
            func(index)
    else:
        lax.fori_loop(0, count, lambda index, carry: (func(index), carry)[1], 0)


def kernel(
    peers,
    slots,
    x_ref,
    src_ref,
    dst_ref,
    rot_ref,
    gain_ref,
    w0_hbm,
    w1_hbm,
    w2_hbm,
    out_ref,
    w0,
    w1,
    w2,
    low_scr,
    high_scr,
    xg,
    own,
    packed,
    other,
    lhs,
    y_scr,
    msg,
    recv,
    rrot,
    mult,
    f_scr,
    back,
    total,
    sq,
    sq_other,
    wsem,
    esem,
    rot_send,
    rot_recv,
    msg_send,
    msg_recv,
    qsem,
):
    me = lax.axis_index("dev")
    half = lax.axis_index("rep")
    nodes = x_ref.shape[0]
    flat = x_ref.shape[1]
    blocks = peers * slots // BLOCK
    group = BLOCK // slots
    partner = {"rep": 1 - half}

    def peer(offset):
        return lax.rem(me + offset, peers)

    weights = [
        pltpu.make_async_copy(src, dst, wsem.at[index])
        for index, (src, dst) in enumerate(((w0_hbm, w0), (w1_hbm, w1), (w2_hbm, w2)))
    ]
    barrier = pltpu.get_barrier_semaphore()
    pl.semaphore_signal(barrier, inc=1, device_id=partner, device_id_type=MESH)
    each(
        peers - 1,
        lambda o: pl.semaphore_signal(
            barrier, inc=1, device_id={"dev": peer(o + 1)}, device_id_type=MESH
        ),
    )
    for copy in weights:
        copy.start()

    lane = lax.broadcasted_iota(jnp.int32, (BLOCK, LANES), 1)
    low_half = lane < HALF
    mine = (lane // HALF) == half

    y_scr[...] = jnp.zeros_like(y_scr)
    xg[:, (TILES - 1) * LANES :] = jnp.zeros((BLOCK, LANES), jnp.float32)
    low_scr[...] = jnp.zeros_like(low_scr)
    high_scr[...] = jnp.zeros_like(high_scr)

    def load_rotation(ref, start):
        for index in range(group):
            rows = ref[start + index].astype(jnp.float32)
            low_scr[index * slots : (index + 1) * slots, 0:WINDOW] = rows[:, 0:WINDOW]
            high_scr[index * slots : (index + 1) * slots, 0:WINDOW] = rows[:, ROT - WINDOW :]
        return low_scr[...], high_scr[...]

    def multiplier(tables, first, second):
        given = [entry for entry in (first, second) if entry is not None]
        which = 0 if max(given) < WINDOW else 1
        shift = which * (ROT - WINDOW)
        places = [WINDOW if e is None else e - shift for e in (first, second)]
        index = jnp.where(low_half, places[0], places[1])
        return jnp.take_along_axis(tables[which], index, axis=1, mode="promise_in_bounds")

    def turn(block):
        tables = load_rotation(rot_ref, block * group)
        rows = pl.multiple_of(block * BLOCK, BLOCK)
        hot = (
            lax.broadcasted_iota(jnp.int32, (BLOCK, nodes), 1) == src_ref[pl.ds(rows, BLOCK), :]
        ).astype(jnp.bfloat16)
        xg[:, 0:flat] = jnp.dot(hot, x_ref[...], preferred_element_type=jnp.float32)
        sums = [None] * FRAME
        for slot, tile, first, second in TERMS:
            part = multiplier(tables, first, second) * xg[:, tile * LANES : (tile + 1) * LANES]
            sums[slot] = part if sums[slot] is None else sums[slot] + part
        for slot in range(FRAME):
            sums[slot] = sums[slot] + pltpu.roll(sums[slot], HALF, 1)
            own[block, :, slot * LANES : (slot + 1) * LANES] = sums[slot]
        for pair in range((FRAME + 1) // 2):
            first = sums[2 * pair]
            second = sums[min(2 * pair + 1, FRAME - 1)]
            packed[block, :, pair * LANES : (pair + 1) * LANES] = jnp.where(
                mine, first, second
            ).astype(jnp.bfloat16)

    each(blocks, turn)

    pl.semaphore_wait(barrier, peers)

    exchange = pltpu.make_async_remote_copy(
        src_ref=packed,
        dst_ref=other,
        send_sem=esem.at[0],
        recv_sem=esem.at[1],
        device_id=partner,
        device_id_type=MESH,
    )
    exchange.start()

    def transfer(source, target, send, receive, o, landing):
        to = peer(o + 1)
        spot = me if landing is None else landing
        return pltpu.make_async_remote_copy(
            src_ref=source.at[to],
            dst_ref=target.at[spot],
            send_sem=send.at[to],
            recv_sem=receive.at[spot],
            device_id={"dev": to},
            device_id_type=MESH,
        )

    def rotations(o, landing=None):
        return transfer(rot_ref, rrot, rot_send, rot_recv, o, landing)

    def messages(o, landing=None):
        return transfer(msg, recv, msg_send, msg_recv, o, landing)

    each(peers - 1, lambda o: rotations(o).start())
    rrot[me] = rot_ref[me]

    for copy in weights:
        copy.wait()
    exchange.wait()

    def mix(block):
        for pair in range((FRAME + 1) // 2):
            there = other[block, :, pair * LANES : (pair + 1) * LANES].astype(jnp.float32)
            for slot, value in ((2 * pair, there), (2 * pair + 1, None)):
                if slot < FRAME:
                    value = pltpu.roll(there, HALF, 1) if value is None else value
                    cols = slice(slot * LANES, (slot + 1) * LANES)
                    lhs[:, cols] = jnp.where(mine, own[block, :, cols], value).astype(jnp.bfloat16)
        nt = (((1,), (1,)), ((), ()))
        y_scr[:, 0 : 7 * HALF] = lax.dot_general(
            lhs[:, 0 : 7 * LANES], w0[...], nt, preferred_element_type=jnp.float32
        )
        for start, count, spots, ref, dims in (
            (7, 6, (512, 896), w1, (((1,), (0,)), ((), ()))),
            (19, 5, (1280, 1664), w2, nt),
        ):
            rows = jnp.concatenate(
                [
                    lhs[:, start * LANES : (start + count) * LANES],
                    lhs[:, (start + count) * LANES : (start + 2 * count) * LANES],
                ],
                axis=0,
            )
            real = lax.dot_general(rows, ref[0], dims, preferred_element_type=jnp.float32)
            imag = lax.dot_general(rows, ref[1], dims, preferred_element_type=jnp.float32)
            width = count * HALF
            y_scr[:, spots[0] : spots[0] + width] = real[:BLOCK] - imag[BLOCK:]
            y_scr[:, spots[1] : spots[1] + width] = imag[:BLOCK] + real[BLOCK:]
        for index in range(group):
            msg[block * group + index] = y_scr[index * slots : (index + 1) * slots, :].astype(
                jnp.bfloat16
            )

    each(blocks, mix)
    each(peers - 1, lambda o: messages(o).start())
    recv[me] = msg[me]

    def wait_rotation(o):
        rotations(o, peer(o + 1)).wait_recv()

    def wait_message(o):
        messages(o, peer(o + 1)).wait_recv()

    each(peers - 1, wait_rotation)

    def prepare(block):
        tables = load_rotation(rrot, block * group)
        for number, (slot, tile, first, second) in enumerate(TERMS):
            mult[number] = multiplier(tables, first, second)

    def collect(block, add):
        for index in range(group):
            f_scr[index * slots : (index + 1) * slots, :] = recv[block * group + index].astype(
                jnp.float32
            )
        doubled = {}
        for slot in range(FRAME):
            tile, side = message_place(slot)
            value = f_scr[:, tile * LANES : (tile + 1) * LANES]
            turned = pltpu.roll(value, HALF, 1)
            doubled[slot] = (
                jnp.where(low_half, value, turned) if side == 0 else jnp.where(low_half, turned, value)
            )
        sums = [None] * TILES
        for number, (slot, tile, first, second) in enumerate(TERMS):
            part = mult[number] * doubled[slot]
            sums[tile] = part if sums[tile] is None else sums[tile] + part
        for tile in range(TILES):
            back[:, tile * LANES : (tile + 1) * LANES] = sums[tile].astype(jnp.bfloat16)
        hot = (
            lax.broadcasted_iota(jnp.int32, (nodes, BLOCK), 0) == dst_ref[pl.ds(block, 1), :]
        ).astype(jnp.bfloat16)
        value = jnp.dot(hot, back[...], preferred_element_type=jnp.float32)
        total[...] = total[...] + value if add else value

    if blocks == 1:
        prepare(0)
        each(peers - 1, wait_message)
        collect(0, False)
    else:
        each(peers - 1, wait_message)
        total[...] = jnp.zeros_like(total)

        def one(block, carry):
            prepare(block)
            collect(block, True)
            return carry

        lax.fori_loop(0, blocks, one, 0)

    partial = None
    for tile in range(TILES):
        value = total[:, tile * LANES : (tile + 1) * LANES]
        partial = value * value if partial is None else partial + value * value
    sq[...] = partial
    share = pltpu.make_async_remote_copy(
        src_ref=sq,
        dst_ref=sq_other,
        send_sem=qsem.at[0],
        recv_sem=qsem.at[1],
        device_id=partner,
        device_id_type=MESH,
    )
    share.start()
    each(peers - 1, lambda o: rotations(o).wait_send())
    each(peers - 1, lambda o: messages(o).wait_send())
    share.wait()
    mean_sq = jnp.sum(sq[...] + sq_other[...], axis=1, keepdims=True) / (2 * flat)
    scale = lax.rsqrt(mean_sq + 1e-06)
    for start in range(0, flat, LANES):
        cols = slice(start, min(start + LANES, flat))
        normed = total[:, cols] * scale
        out_ref[:, cols] = (
            x_ref[:, cols].astype(jnp.float32) + gain_ref[:, cols] * normed
        ).astype(jnp.bfloat16)


def shards(node_features, src_node, dst_node, counts, rotation, w_zero, w_one, w_two, norm_gain):
    nodes, _, flat = node_features.shape
    peers, slots = src_node.shape[1:]
    edges = peers * slots
    blocks = edges // BLOCK
    x = node_features.reshape(nodes, flat)
    live = jnp.arange(slots)[None, :] < counts.reshape(peers)[:, None]
    src = jnp.where(live, src_node.reshape(peers, slots), -1).reshape(edges, 1)
    dst = dst_node.reshape(blocks, BLOCK)
    rot = rotation.reshape(peers, slots, ROT)
    w0 = w_zero.reshape(w_zero.shape[0], -1).T
    w1 = w_one.reshape(2, w_one.shape[1], -1)
    w2 = w_two.reshape(2, w_two.shape[1], -1).swapaxes(1, 2)
    vmem = pl.BlockSpec(memory_space=pltpu.VMEM)
    hbm = pl.BlockSpec(memory_space=pl.ANY)
    f32, bf16 = jnp.float32, jnp.bfloat16
    dma = pltpu.SemaphoreType.DMA
    pairs = (FRAME + 1) // 2
    out = pl.pallas_call(
        functools.partial(kernel, peers, slots),
        out_shape=jax.ShapeDtypeStruct((nodes, flat), bf16),
        in_specs=[vmem] * 5 + [hbm] * 3,
        out_specs=vmem,
        scratch_shapes=[
            pltpu.VMEM(w0.shape, bf16),
            pltpu.VMEM(w1.shape, bf16),
            pltpu.VMEM(w2.shape, bf16),
            pltpu.VMEM((BLOCK, LANES), f32),
            pltpu.VMEM((BLOCK, LANES), f32),
            pltpu.VMEM((BLOCK, WIDE), f32),
            pltpu.VMEM((blocks, BLOCK, FRAME * LANES), f32),
            pltpu.VMEM((blocks, BLOCK, pairs * LANES), bf16),
            pltpu.VMEM((blocks, BLOCK, pairs * LANES), bf16),
            pltpu.VMEM((BLOCK, FRAME * LANES), bf16),
            pltpu.VMEM((BLOCK, MESSAGE), f32),
            pltpu.VMEM((peers, slots, MESSAGE), bf16),
            pltpu.VMEM((peers, slots, MESSAGE), bf16),
            pltpu.VMEM((peers, slots, ROT), bf16),
            pltpu.VMEM((len(TERMS), BLOCK, LANES), f32),
            pltpu.VMEM((BLOCK, MESSAGE), f32),
            pltpu.VMEM((BLOCK, WIDE), bf16),
            pltpu.VMEM((nodes, WIDE), f32),
            pltpu.VMEM((nodes, LANES), f32),
            pltpu.VMEM((nodes, LANES), f32),
            dma((3,)),
            dma((2,)),
            dma((peers,)),
            dma((peers,)),
            dma((peers,)),
            dma((peers,)),
            dma((2,)),
        ],
        compiler_params=pltpu.CompilerParams(
            collective_id=0, has_side_effects=True, vmem_limit_bytes=40 * 1024 * 1024
        ),
    )(x, src, dst, rot, norm_gain, w0, w1, w2)
    return out.reshape(nodes, 1, flat)


def solution(mesh):
    return jax.shard_map(
        shards,
        mesh=mesh,
        in_specs=(
            P("dev", "rep", None),
            P("dev", None, None),
            P("dev", None, None),
            P("dev", None),
            P("dev", None, None, None),
            P(None, "rep", None),
            P(None, None, "rep", None),
            P(None, None, "rep", None),
            P("rep", None),
        ),
        out_specs=P("dev", "rep", None),
        check_vma=False,
    )
```

```python
import functools

import jax
import jax.numpy as jnp
from jax import lax
from jax.experimental import pallas as pl
from jax.experimental.pallas import tpu as pltpu
from jax.sharding import PartitionSpec as P

LANES = 128
HALF = 64
COEFFS = 49
FRAME = 29
ROT = 235
WINDOW = 120
TILES = (COEFFS + 1) // 2
WIDE = TILES * LANES
GROUPS = ((0, 7, 0), (7, 6, 512), (13, 6, 896), (19, 5, 1280), (24, 5, 1664))
MESSAGE = 2048
VMEM_LIMIT = 67043328
BLOCK = 32
MESH = pl.DeviceIdType.MESH


def frame_slot(degree, order):
    if order == 0:
        return degree
    if order == 1:
        return 6 + degree
    if order == -1:
        return 12 + degree
    if order == 2:
        return 17 + degree
    return 22 + degree


def terms():
    listing = []
    spot = 0
    for degree in range(7):
        reach = min(degree, 2)
        span = 2 * degree + 1
        first = degree * degree
        for row in range(2 * reach + 1):
            slot = frame_slot(degree, row - reach)
            for tile in range(first // 2, (first + span - 1) // 2 + 1):
                ends = []
                for coeff in (2 * tile, 2 * tile + 1):
                    inside = first <= coeff < first + span
                    ends.append(spot + row * span + coeff - first if inside else None)
                listing.append((slot, tile, ends[0], ends[1]))
        spot += span * (2 * reach + 1)
    return listing


TERMS = terms()


def message_place(slot):
    for first, count, base in GROUPS:
        if first <= slot < first + count:
            lane = base + (slot - first) * HALF
            return lane // LANES, (lane % LANES) // HALF
    raise ValueError


def each(count, func):
    if count <= 16:
        for index in range(count):
            func(index)
    else:
        lax.fori_loop(0, count, lambda index, carry: (func(index), carry)[1], 0)


def kernel(
    peers,
    slots,
    x_hbm,
    rot_hbm,
    src_hbm,
    cnt_hbm,
    dst_hbm,
    gain_hbm,
    w0_hbm,
    w1_hbm,
    w2_hbm,
    out_ref,
    x_ref,
    rot_ref,
    src_ref,
    cnt_ref,
    dst_ref,
    gain_ref,
    w0,
    w1,
    w2,
    low_scr,
    high_scr,
    xg,
    own,
    packed,
    other,
    lhs,
    y_scr,
    msg,
    recv,
    rrot,
    mult,
    f_scr,
    back,
    total,
    sq,
    sq_other,
    wsem,
    esem,
    rot_send,
    rot_recv,
    msg_send,
    msg_recv,
    qsem,
):
    me = lax.axis_index("dev")
    half = lax.axis_index("rep")
    nodes = x_ref.shape[0]
    flat = x_ref.shape[1]
    blocks = peers * slots // BLOCK
    group = BLOCK // slots
    partner = {"rep": 1 - half}

    def peer(offset):
        return lax.rem(me + offset, peers)

    loads = [
        pltpu.make_async_copy(src, dst, wsem.at[index])
        for index, (src, dst) in enumerate(
            (
                (x_hbm, x_ref),
                (rot_hbm, rot_ref),
                (src_hbm, src_ref),
                (cnt_hbm, cnt_ref),
                (dst_hbm, dst_ref),
                (gain_hbm, gain_ref),
                (w0_hbm, w0),
                (w1_hbm, w1),
                (w2_hbm, w2),
            )
        )
    ]
    for copy in loads:
        copy.start()
    barrier = pltpu.get_barrier_semaphore()
    pl.semaphore_signal(barrier, inc=1, device_id=partner, device_id_type=MESH)
    each(
        peers - 1,
        lambda o: pl.semaphore_signal(
            barrier, inc=1, device_id={"dev": peer(o + 1)}, device_id_type=MESH
        ),
    )

    lane = lax.broadcasted_iota(jnp.int32, (BLOCK, LANES), 1)
    low_half = lane < HALF
    mine = (lane // HALF) == half

    y_scr[...] = jnp.zeros_like(y_scr)
    xg[:, (TILES - 1) * LANES :] = jnp.zeros((BLOCK, LANES), jnp.float32)
    low_scr[...] = jnp.zeros_like(low_scr)
    high_scr[...] = jnp.zeros_like(high_scr)

    def column(rows):
        row = lax.broadcasted_iota(jnp.int32, (BLOCK, group), 0)
        spot = lax.broadcasted_iota(jnp.int32, (BLOCK, group), 1)
        chosen = jnp.zeros((BLOCK, group), jnp.float32)
        for index in range(slots):
            chosen = jnp.where(row == spot * slots + index, rows[index], chosen)
        return jnp.sum(chosen, axis=1, keepdims=True)

    def sources(block):
        count = cnt_ref[block]
        value = src_ref[block]
        return column(
            [
                jnp.where(count > index, value[index : index + 1], -1).astype(jnp.float32)
                for index in range(slots)
            ]
        )

    def targets(block):
        value = dst_ref[block].astype(jnp.float32)
        down = column([value[index : index + 1] for index in range(slots)])
        row = lax.broadcasted_iota(jnp.int32, (BLOCK, BLOCK), 0)
        spot = lax.broadcasted_iota(jnp.int32, (BLOCK, BLOCK), 1)
        return jnp.sum(jnp.where(row == spot, down, 0.0), axis=0, keepdims=True)

    def load_rotation(ref, start):
        for index in range(group):
            rows = ref[start + index].astype(jnp.float32)
            low_scr[index * slots : (index + 1) * slots, 0:WINDOW] = rows[:, 0:WINDOW]
            high_scr[index * slots : (index + 1) * slots, 0:WINDOW] = rows[:, ROT - WINDOW :]
        return low_scr[...], high_scr[...]

    def multiplier(tables, first, second):
        given = [entry for entry in (first, second) if entry is not None]
        which = 0 if max(given) < WINDOW else 1
        shift = which * (ROT - WINDOW)
        places = [WINDOW if e is None else e - shift for e in (first, second)]
        index = jnp.where(low_half, places[0], places[1])
        return jnp.take_along_axis(tables[which], index, axis=1, mode="promise_in_bounds")

    def turn(block):
        tables = load_rotation(rot_ref, block * group)
        hot = (
            lax.broadcasted_iota(jnp.int32, (BLOCK, nodes), 1).astype(jnp.float32) == sources(block)
        ).astype(jnp.bfloat16)
        xg[:, 0:flat] = jnp.dot(hot, x_ref[...], preferred_element_type=jnp.float32)
        sums = [None] * FRAME
        for slot, tile, first, second in TERMS:
            part = multiplier(tables, first, second) * xg[:, tile * LANES : (tile + 1) * LANES]
            sums[slot] = part if sums[slot] is None else sums[slot] + part
        for slot in range(FRAME):
            sums[slot] = sums[slot] + pltpu.roll(sums[slot], HALF, 1)
            own[block, :, slot * LANES : (slot + 1) * LANES] = sums[slot]
        for pair in range((FRAME + 1) // 2):
            first = sums[2 * pair]
            second = sums[min(2 * pair + 1, FRAME - 1)]
            packed[block, :, pair * LANES : (pair + 1) * LANES] = jnp.where(
                mine, first, second
            ).astype(jnp.bfloat16)

    for copy in loads[:4]:
        copy.wait()
    each(blocks, turn)

    pl.semaphore_wait(barrier, peers)

    exchange = pltpu.make_async_remote_copy(
        src_ref=packed,
        dst_ref=other,
        send_sem=esem.at[0],
        recv_sem=esem.at[1],
        device_id=partner,
        device_id_type=MESH,
    )
    exchange.start()

    def transfer(source, target, send, receive, o, landing):
        to = peer(o + 1)
        spot = me if landing is None else landing
        return pltpu.make_async_remote_copy(
            src_ref=source.at[to],
            dst_ref=target.at[spot],
            send_sem=send.at[to],
            recv_sem=receive.at[spot],
            device_id={"dev": to},
            device_id_type=MESH,
        )

    def rotations(o, landing=None):
        return transfer(rot_ref, rrot, rot_send, rot_recv, o, landing)

    def messages(o, landing=None):
        return transfer(msg, recv, msg_send, msg_recv, o, landing)

    each(peers - 1, lambda o: rotations(o).start())
    rrot[me] = rot_ref[me]

    for copy in loads[4:]:
        copy.wait()
    exchange.wait()

    def mix(block):
        for pair in range((FRAME + 1) // 2):
            there = other[block, :, pair * LANES : (pair + 1) * LANES].astype(jnp.float32)
            for slot, value in ((2 * pair, there), (2 * pair + 1, None)):
                if slot < FRAME:
                    value = pltpu.roll(there, HALF, 1) if value is None else value
                    cols = slice(slot * LANES, (slot + 1) * LANES)
                    lhs[:, cols] = jnp.where(mine, own[block, :, cols], value).astype(jnp.bfloat16)
        nt = (((1,), (1,)), ((), ()))
        y_scr[:, 0 : 7 * HALF] = lax.dot_general(
            lhs[:, 0 : 7 * LANES], w0[...], nt, preferred_element_type=jnp.float32
        )
        for start, count, spots, ref, dims in (
            (7, 6, (512, 896), w1, (((1,), (0,)), ((), ()))),
            (19, 5, (1280, 1664), w2, nt),
        ):
            rows = jnp.concatenate(
                [
                    lhs[:, start * LANES : (start + count) * LANES],
                    lhs[:, (start + count) * LANES : (start + 2 * count) * LANES],
                ],
                axis=0,
            )
            real = lax.dot_general(rows, ref[0], dims, preferred_element_type=jnp.float32)
            imag = lax.dot_general(rows, ref[1], dims, preferred_element_type=jnp.float32)
            width = count * HALF
            y_scr[:, spots[0] : spots[0] + width] = real[:BLOCK] - imag[BLOCK:]
            y_scr[:, spots[1] : spots[1] + width] = imag[:BLOCK] + real[BLOCK:]
        for index in range(group):
            msg[block * group + index] = y_scr[index * slots : (index + 1) * slots, :].astype(
                jnp.bfloat16
            )

    each(blocks, mix)
    each(peers - 1, lambda o: messages(o).start())
    recv[me] = msg[me]

    def wait_rotation(o):
        rotations(o, peer(o + 1)).wait_recv()

    def wait_message(o):
        messages(o, peer(o + 1)).wait_recv()

    each(peers - 1, wait_rotation)

    def prepare(block):
        tables = load_rotation(rrot, block * group)
        for number, (slot, tile, first, second) in enumerate(TERMS):
            mult[number] = multiplier(tables, first, second)

    def collect(block, add):
        for index in range(group):
            f_scr[index * slots : (index + 1) * slots, :] = recv[block * group + index].astype(
                jnp.float32
            )
        doubled = {}
        for slot in range(FRAME):
            tile, side = message_place(slot)
            value = f_scr[:, tile * LANES : (tile + 1) * LANES]
            turned = pltpu.roll(value, HALF, 1)
            doubled[slot] = (
                jnp.where(low_half, value, turned) if side == 0 else jnp.where(low_half, turned, value)
            )
        sums = [None] * TILES
        for number, (slot, tile, first, second) in enumerate(TERMS):
            part = mult[number] * doubled[slot]
            sums[tile] = part if sums[tile] is None else sums[tile] + part
        for tile in range(TILES):
            back[:, tile * LANES : (tile + 1) * LANES] = sums[tile].astype(jnp.bfloat16)
        hot = (
            lax.broadcasted_iota(jnp.int32, (nodes, BLOCK), 0).astype(jnp.float32) == targets(block)
        ).astype(jnp.bfloat16)
        value = jnp.dot(hot, back[...], preferred_element_type=jnp.float32)
        total[...] = total[...] + value if add else value

    if blocks == 1:
        prepare(0)
        each(peers - 1, wait_message)
        collect(0, False)
    else:
        each(peers - 1, wait_message)
        total[...] = jnp.zeros_like(total)

        def one(block, carry):
            prepare(block)
            collect(block, True)
            return carry

        lax.fori_loop(0, blocks, one, 0)

    partial = None
    for tile in range(TILES):
        value = total[:, tile * LANES : (tile + 1) * LANES]
        partial = value * value if partial is None else partial + value * value
    sq[...] = partial
    share = pltpu.make_async_remote_copy(
        src_ref=sq,
        dst_ref=sq_other,
        send_sem=qsem.at[0],
        recv_sem=qsem.at[1],
        device_id=partner,
        device_id_type=MESH,
    )
    share.start()
    each(peers - 1, lambda o: rotations(o).wait_send())
    each(peers - 1, lambda o: messages(o).wait_send())
    share.wait()
    mean_sq = jnp.sum(sq[...] + sq_other[...], axis=1, keepdims=True) / (2 * flat)
    scale = lax.rsqrt(mean_sq + 1e-06)
    for start in range(0, flat, LANES):
        cols = slice(start, min(start + LANES, flat))
        normed = total[:, cols] * scale
        out_ref[:, cols] = (
            x_ref[:, cols].astype(jnp.float32) + gain_ref[:, cols] * normed
        ).astype(jnp.bfloat16)


def shards(node_features, src_node, dst_node, counts, rotation, w_zero, w_one, w_two, norm_gain):
    nodes, _, flat = node_features.shape
    peers, slots = src_node.shape[1:]
    edges = peers * slots
    blocks = edges // BLOCK
    x = node_features.reshape(nodes, flat)
    group = peers // blocks
    src = src_node.reshape(blocks, group, slots).swapaxes(1, 2)
    dst = dst_node.reshape(blocks, group, slots).swapaxes(1, 2)
    cnt = counts.reshape(blocks, 1, group)
    rot = rotation.reshape(peers, slots, ROT)
    w0 = w_zero.reshape(w_zero.shape[0], -1).T
    w1 = w_one.reshape(2, w_one.shape[1], -1)
    w2 = w_two.reshape(2, w_two.shape[1], -1).swapaxes(1, 2)
    vmem = pl.BlockSpec(memory_space=pltpu.VMEM)
    hbm = pl.BlockSpec(memory_space=pl.ANY)
    f32, bf16 = jnp.float32, jnp.bfloat16
    dma = pltpu.SemaphoreType.DMA
    pairs = (FRAME + 1) // 2
    out = pl.pallas_call(
        functools.partial(kernel, peers, slots),
        out_shape=jax.ShapeDtypeStruct((nodes, flat), bf16),
        in_specs=[hbm] * 9,
        out_specs=vmem,
        scratch_shapes=[
            pltpu.VMEM(x.shape, bf16),
            pltpu.VMEM(rot.shape, bf16),
            pltpu.VMEM(src.shape, jnp.int32),
            pltpu.VMEM(cnt.shape, jnp.int32),
            pltpu.VMEM(dst.shape, jnp.int32),
            pltpu.VMEM(norm_gain.shape, f32),
            pltpu.VMEM(w0.shape, bf16),
            pltpu.VMEM(w1.shape, bf16),
            pltpu.VMEM(w2.shape, bf16),
            pltpu.VMEM((BLOCK, LANES), f32),
            pltpu.VMEM((BLOCK, LANES), f32),
            pltpu.VMEM((BLOCK, WIDE), f32),
            pltpu.VMEM((blocks, BLOCK, FRAME * LANES), f32),
            pltpu.VMEM((blocks, BLOCK, pairs * LANES), bf16),
            pltpu.VMEM((blocks, BLOCK, pairs * LANES), bf16),
            pltpu.VMEM((BLOCK, FRAME * LANES), bf16),
            pltpu.VMEM((BLOCK, MESSAGE), f32),
            pltpu.VMEM((peers, slots, MESSAGE), bf16),
            pltpu.VMEM((peers, slots, MESSAGE), bf16),
            pltpu.VMEM((peers, slots, ROT), bf16),
            pltpu.VMEM((len(TERMS), BLOCK, LANES), f32),
            pltpu.VMEM((BLOCK, MESSAGE), f32),
            pltpu.VMEM((BLOCK, WIDE), bf16),
            pltpu.VMEM((nodes, WIDE), f32),
            pltpu.VMEM((nodes, LANES), f32),
            pltpu.VMEM((nodes, LANES), f32),
            dma((9,)),
            dma((2,)),
            dma((peers,)),
            dma((peers,)),
            dma((peers,)),
            dma((peers,)),
            dma((2,)),
        ],
        compiler_params=pltpu.CompilerParams(
            collective_id=0, has_side_effects=True, vmem_limit_bytes=VMEM_LIMIT
        ),
    )(x, rot, src, cnt, dst, norm_gain, w0, w1, w2)
    return out.reshape(nodes, 1, flat)


def solution(mesh):
    return jax.shard_map(
        shards,
        mesh=mesh,
        in_specs=(
            P("dev", "rep", None),
            P("dev", None, None),
            P("dev", None, None),
            P("dev", None),
            P("dev", None, None, None),
            P(None, "rep", None),
            P(None, None, "rep", None),
            P(None, None, "rep", None),
            P("rep", None),
        ),
        out_specs=P("dev", "rep", None),
        check_vma=False,
    )
```

```python
import functools

import jax
import jax.numpy as jnp
from jax import lax
from jax.experimental import pallas as pl
from jax.experimental.pallas import tpu as pltpu
from jax.sharding import PartitionSpec as P

LANES = 128
HALF = 64
COEFFS = 49
FRAME = 29
ROT = 235
WINDOW = 120
TILES = (COEFFS + 1) // 2
WIDE = TILES * LANES
MESSAGE = (FRAME + 1) // 2 * LANES
VMEM_LIMIT = 40 * 1024 * 1024
BLOCK = 32
MESH = pl.DeviceIdType.MESH


def frame_slot(degree, order):
    if order == 0:
        return degree
    if order == 1:
        return 6 + degree
    if order == -1:
        return 12 + degree
    if order == 2:
        return 17 + degree
    return 22 + degree


def terms():
    listing = []
    spot = 0
    for degree in range(7):
        reach = min(degree, 2)
        span = 2 * degree + 1
        first = degree * degree
        for row in range(2 * reach + 1):
            slot = frame_slot(degree, row - reach)
            for tile in range(first // 2, (first + span - 1) // 2 + 1):
                ends = []
                for coeff in (2 * tile, 2 * tile + 1):
                    inside = first <= coeff < first + span
                    ends.append(spot + row * span + coeff - first if inside else None)
                listing.append((slot, tile, ends[0], ends[1]))
        spot += span * (2 * reach + 1)
    return listing


TERMS = terms()


def message_place(slot):
    return slot // 2, slot % 2


def far_first(count):
    return sorted(range(1, count), key=lambda offset: -min(offset, count - offset))


def each_peer(count, func):
    if count <= 17:
        for offset in far_first(count):
            func(offset - 1)
    else:
        each(count - 1, func)


def each(count, func):
    if count <= 16:
        for index in range(count):
            func(index)
    else:
        lax.fori_loop(0, count, lambda index, carry: (func(index), carry)[1], 0)


def kernel(
    peers,
    slots,
    x_hbm,
    rot_hbm,
    src_hbm,
    cnt_hbm,
    dst_hbm,
    gain_hbm,
    w0_hbm,
    w1_hbm,
    w2_hbm,
    out_ref,
    x_ref,
    rot_ref,
    src_ref,
    cnt_ref,
    dst_ref,
    gain_ref,
    w0,
    w1,
    w2,
    low_scr,
    high_scr,
    xg,
    own,
    packed,
    other,
    lhs,
    y_scr,
    msg,
    recv,
    rrot,
    mult,
    f_scr,
    back,
    total,
    sq,
    sq_other,
    wsem,
    esem,
    rot_send,
    rot_recv,
    msg_send,
    msg_recv,
    qsem,
):
    me = lax.axis_index("dev")
    half = lax.axis_index("rep")
    nodes = x_ref.shape[0]
    flat = x_ref.shape[1]
    blocks = peers * slots // BLOCK
    group = BLOCK // slots
    partner = {"rep": 1 - half}

    def peer(offset):
        return lax.rem(me + offset, peers)

    loads = [
        pltpu.make_async_copy(src, dst, wsem.at[index])
        for index, (src, dst) in enumerate(
            (
                (x_hbm, x_ref),
                (rot_hbm, rot_ref),
                (src_hbm, src_ref),
                (cnt_hbm, cnt_ref),
                (dst_hbm, dst_ref),
                (gain_hbm, gain_ref),
                (w0_hbm, w0),
                (w1_hbm, w1),
                (w2_hbm, w2),
            )
        )
    ]
    for copy in loads:
        copy.start()
    barrier = pltpu.get_barrier_semaphore()
    pl.semaphore_signal(barrier, inc=1, device_id=partner, device_id_type=MESH)
    each(
        peers - 1,
        lambda o: pl.semaphore_signal(
            barrier, inc=1, device_id={"dev": peer(o + 1)}, device_id_type=MESH
        ),
    )

    lane = lax.broadcasted_iota(jnp.int32, (BLOCK, LANES), 1)
    low_half = lane < HALF
    mine = (lane // HALF) == half

    y_scr[...] = jnp.zeros_like(y_scr)
    xg[:, (TILES - 1) * LANES :] = jnp.zeros((BLOCK, LANES), jnp.float32)
    low_scr[...] = jnp.zeros_like(low_scr)
    high_scr[...] = jnp.zeros_like(high_scr)

    def column(rows):
        row = lax.broadcasted_iota(jnp.int32, (BLOCK, group), 0)
        spot = lax.broadcasted_iota(jnp.int32, (BLOCK, group), 1)
        chosen = jnp.zeros((BLOCK, group), jnp.float32)
        for index in range(slots):
            chosen = jnp.where(row == spot * slots + index, rows[index], chosen)
        return jnp.sum(chosen, axis=1, keepdims=True)

    def sources(block):
        count = cnt_ref[block]
        value = src_ref[block]
        return column(
            [
                jnp.where(count > index, value[index : index + 1], -1).astype(jnp.float32)
                for index in range(slots)
            ]
        )

    def targets(block):
        value = dst_ref[block].astype(jnp.float32)
        down = column([value[index : index + 1] for index in range(slots)])
        row = lax.broadcasted_iota(jnp.int32, (BLOCK, BLOCK), 0)
        spot = lax.broadcasted_iota(jnp.int32, (BLOCK, BLOCK), 1)
        return jnp.sum(jnp.where(row == spot, down, 0.0), axis=0, keepdims=True)

    def load_rotation(ref, start):
        for index in range(group):
            rows = ref[start + index].astype(jnp.float32)
            low_scr[index * slots : (index + 1) * slots, 0:WINDOW] = rows[:, 0:WINDOW]
            high_scr[index * slots : (index + 1) * slots, 0:WINDOW] = rows[:, ROT - WINDOW :]
        return low_scr[...], high_scr[...]

    def multiplier(tables, first, second):
        given = [entry for entry in (first, second) if entry is not None]
        which = 0 if max(given) < WINDOW else 1
        shift = which * (ROT - WINDOW)
        places = [WINDOW if e is None else e - shift for e in (first, second)]
        index = jnp.where(low_half, places[0], places[1])
        return jnp.take_along_axis(tables[which], index, axis=1, mode="promise_in_bounds")

    def turn(block):
        tables = load_rotation(rot_ref, block * group)
        hot = (
            lax.broadcasted_iota(jnp.int32, (BLOCK, nodes), 1).astype(jnp.float32) == sources(block)
        ).astype(jnp.bfloat16)
        xg[:, 0:flat] = jnp.dot(hot, x_ref[...], preferred_element_type=jnp.float32)
        sums = [None] * FRAME
        for slot, tile, first, second in TERMS:
            part = multiplier(tables, first, second) * xg[:, tile * LANES : (tile + 1) * LANES]
            sums[slot] = part if sums[slot] is None else sums[slot] + part
        for slot in range(FRAME):
            sums[slot] = sums[slot] + pltpu.roll(sums[slot], HALF, 1)
            own[block, :, slot * LANES : (slot + 1) * LANES] = sums[slot]
        for pair in range((FRAME + 1) // 2):
            first = sums[2 * pair]
            second = sums[min(2 * pair + 1, FRAME - 1)]
            packed[block, :, pair * LANES : (pair + 1) * LANES] = jnp.where(
                mine, first, second
            ).astype(jnp.bfloat16)

    for copy in loads[:4]:
        copy.wait()
    each(blocks, turn)

    pl.semaphore_wait(barrier, peers)

    exchange = pltpu.make_async_remote_copy(
        src_ref=packed,
        dst_ref=other,
        send_sem=esem.at[0],
        recv_sem=esem.at[1],
        device_id=partner,
        device_id_type=MESH,
    )
    exchange.start()

    def transfer(source, target, send, receive, o, landing):
        to = peer(o + 1)
        spot = me if landing is None else landing
        return pltpu.make_async_remote_copy(
            src_ref=source.at[to],
            dst_ref=target.at[spot],
            send_sem=send.at[to],
            recv_sem=receive.at[spot],
            device_id={"dev": to},
            device_id_type=MESH,
        )

    def rotations(o, landing=None):
        return transfer(rot_ref, rrot, rot_send, rot_recv, o, landing)

    def messages(o, landing=None):
        return transfer(msg, recv, msg_send, msg_recv, o, landing)

    each_peer(peers, lambda o: rotations(o).start())
    rrot[me] = rot_ref[me]

    for copy in loads[4:]:
        copy.wait()
    exchange.wait()

    def mix(block):
        for pair in range((FRAME + 1) // 2):
            there = other[block, :, pair * LANES : (pair + 1) * LANES].astype(jnp.float32)
            for slot, value in ((2 * pair, there), (2 * pair + 1, None)):
                if slot < FRAME:
                    value = pltpu.roll(there, HALF, 1) if value is None else value
                    cols = slice(slot * LANES, (slot + 1) * LANES)
                    lhs[:, cols] = jnp.where(mine, own[block, :, cols], value).astype(jnp.bfloat16)
        nt = (((1,), (1,)), ((), ()))
        y_scr[:, 0 : 7 * HALF] = lax.dot_general(
            lhs[:, 0 : 7 * LANES], w0[...], nt, preferred_element_type=jnp.float32
        )
        for start, count, ref, dims in (
            (7, 6, w1, (((1,), (0,)), ((), ()))),
            (19, 5, w2, nt),
        ):
            rows = jnp.concatenate(
                [
                    lhs[:, start * LANES : (start + count) * LANES],
                    lhs[:, (start + count) * LANES : (start + 2 * count) * LANES],
                ],
                axis=0,
            )
            real = lax.dot_general(rows, ref[0], dims, preferred_element_type=jnp.float32)
            imag = lax.dot_general(rows, ref[1], dims, preferred_element_type=jnp.float32)
            width = count * HALF
            plus = start * HALF
            minus = plus + width
            y_scr[:, plus : plus + width] = real[:BLOCK] - imag[BLOCK:]
            y_scr[:, minus : minus + width] = imag[:BLOCK] + real[BLOCK:]
        for index in range(group):
            msg[block * group + index] = y_scr[index * slots : (index + 1) * slots, :].astype(
                jnp.bfloat16
            )

    each(blocks, mix)
    each_peer(peers, lambda o: messages(o).start())
    recv[me] = msg[me]

    def wait_rotation(o):
        rotations(o, peer(o + 1)).wait_recv()

    def wait_message(o):
        messages(o, peer(o + 1)).wait_recv()

    each(peers - 1, wait_rotation)

    def prepare(block):
        tables = load_rotation(rrot, block * group)
        for number, (slot, tile, first, second) in enumerate(TERMS):
            mult[number] = multiplier(tables, first, second)

    def collect(block, add):
        for index in range(group):
            f_scr[index * slots : (index + 1) * slots, :] = recv[block * group + index].astype(
                jnp.float32
            )
        doubled = {}
        for slot in range(FRAME):
            tile, side = message_place(slot)
            value = f_scr[:, tile * LANES : (tile + 1) * LANES]
            turned = pltpu.roll(value, HALF, 1)
            doubled[slot] = (
                jnp.where(low_half, value, turned) if side == 0 else jnp.where(low_half, turned, value)
            )
        sums = [None] * TILES
        for number, (slot, tile, first, second) in enumerate(TERMS):
            part = mult[number] * doubled[slot]
            sums[tile] = part if sums[tile] is None else sums[tile] + part
        for tile in range(TILES):
            back[:, tile * LANES : (tile + 1) * LANES] = sums[tile].astype(jnp.bfloat16)
        hot = (
            lax.broadcasted_iota(jnp.int32, (nodes, BLOCK), 0).astype(jnp.float32) == targets(block)
        ).astype(jnp.bfloat16)
        value = jnp.dot(hot, back[...], preferred_element_type=jnp.float32)
        total[...] = total[...] + value if add else value

    if blocks == 1:
        prepare(0)
        each(peers - 1, wait_message)
        collect(0, False)
    else:
        each(peers - 1, wait_message)
        total[...] = jnp.zeros_like(total)

        def one(block, carry):
            prepare(block)
            collect(block, True)
            return carry

        lax.fori_loop(0, blocks, one, 0)

    partial = None
    for tile in range(TILES):
        value = total[:, tile * LANES : (tile + 1) * LANES]
        partial = value * value if partial is None else partial + value * value
    sq[...] = partial
    share = pltpu.make_async_remote_copy(
        src_ref=sq,
        dst_ref=sq_other,
        send_sem=qsem.at[0],
        recv_sem=qsem.at[1],
        device_id=partner,
        device_id_type=MESH,
    )
    share.start()
    each(peers - 1, lambda o: rotations(o).wait_send())
    each(peers - 1, lambda o: messages(o).wait_send())
    share.wait()
    mean_sq = jnp.sum(sq[...] + sq_other[...], axis=1, keepdims=True) / (2 * flat)
    scale = lax.rsqrt(mean_sq + 1e-06)
    for start in range(0, flat, LANES):
        cols = slice(start, min(start + LANES, flat))
        normed = total[:, cols] * scale
        out_ref[:, cols] = (
            x_ref[:, cols].astype(jnp.float32) + gain_ref[:, cols] * normed
        ).astype(jnp.bfloat16)


def shards(node_features, src_node, dst_node, counts, rotation, w_zero, w_one, w_two, norm_gain):
    nodes, _, flat = node_features.shape
    peers, slots = src_node.shape[1:]
    edges = peers * slots
    blocks = edges // BLOCK
    x = node_features.reshape(nodes, flat)
    group = peers // blocks
    src = src_node.reshape(blocks, group, slots).swapaxes(1, 2)
    dst = dst_node.reshape(blocks, group, slots).swapaxes(1, 2)
    cnt = counts.reshape(blocks, 1, group)
    rot = rotation.reshape(peers, slots, ROT)
    w0 = w_zero.reshape(w_zero.shape[0], -1).T
    w1 = w_one.reshape(2, w_one.shape[1], -1)
    w2 = w_two.reshape(2, w_two.shape[1], -1).swapaxes(1, 2)
    vmem = pl.BlockSpec(memory_space=pltpu.VMEM)
    hbm = pl.BlockSpec(memory_space=pltpu.HBM)
    f32, bf16 = jnp.float32, jnp.bfloat16
    dma = pltpu.SemaphoreType.DMA
    pairs = (FRAME + 1) // 2
    operands = (x, rot, src, cnt, dst, norm_gain, w0, w1, w2)
    out = pl.pallas_call(
        functools.partial(kernel, peers, slots),
        out_shape=jax.ShapeDtypeStruct((nodes, flat), bf16),
        in_specs=[hbm] * 9,
        out_specs=vmem,
        scratch_shapes=[
            pltpu.VMEM(x.shape, bf16),
            pltpu.VMEM(rot.shape, bf16),
            pltpu.VMEM(src.shape, jnp.int32),
            pltpu.VMEM(cnt.shape, jnp.int32),
            pltpu.VMEM(dst.shape, jnp.int32),
            pltpu.VMEM(norm_gain.shape, f32),
            pltpu.VMEM(w0.shape, bf16),
            pltpu.VMEM(w1.shape, bf16),
            pltpu.VMEM(w2.shape, bf16),
            pltpu.VMEM((BLOCK, LANES), f32),
            pltpu.VMEM((BLOCK, LANES), f32),
            pltpu.VMEM((BLOCK, WIDE), f32),
            pltpu.VMEM((blocks, BLOCK, FRAME * LANES), f32),
            pltpu.VMEM((blocks, BLOCK, pairs * LANES), bf16),
            pltpu.VMEM((blocks, BLOCK, pairs * LANES), bf16),
            pltpu.VMEM((BLOCK, FRAME * LANES), bf16),
            pltpu.VMEM((BLOCK, MESSAGE), f32),
            pltpu.VMEM((peers, slots, MESSAGE), bf16),
            pltpu.VMEM((peers, slots, MESSAGE), bf16),
            pltpu.VMEM((peers, slots, ROT), bf16),
            pltpu.VMEM((len(TERMS), BLOCK, LANES), f32),
            pltpu.VMEM((BLOCK, MESSAGE), f32),
            pltpu.VMEM((BLOCK, WIDE), bf16),
            pltpu.VMEM((nodes, WIDE), f32),
            pltpu.VMEM((nodes, LANES), f32),
            pltpu.VMEM((nodes, LANES), f32),
            dma((9,)),
            dma((2,)),
            dma((peers,)),
            dma((peers,)),
            dma((peers,)),
            dma((peers,)),
            dma((2,)),
        ],
        compiler_params=pltpu.CompilerParams(
            collective_id=0, has_side_effects=True, vmem_limit_bytes=VMEM_LIMIT
        ),
    )(*(pltpu.with_memory_space_constraint(operand, pltpu.HBM) for operand in operands))
    return out.reshape(nodes, 1, flat)


def solution(mesh):
    return jax.shard_map(
        shards,
        mesh=mesh,
        in_specs=(
            P("dev", "rep", None),
            P("dev", None, None),
            P("dev", None, None),
            P("dev", None),
            P("dev", None, None, None),
            P(None, "rep", None),
            P(None, None, "rep", None),
            P(None, None, "rep", None),
            P("rep", None),
        ),
        out_specs=P("dev", "rep", None),
        check_vma=False,
    )
```

```python
import functools

import jax
import jax.numpy as jnp
from jax import lax
from jax.experimental import pallas as pl
from jax.experimental.pallas import tpu as pltpu
from jax.sharding import PartitionSpec as P

LANES = 128
HALF = 64
COEFFS = 49
FRAME = 29
ROT = 235
WINDOW = 120
TILES = (COEFFS + 1) // 2
WIDE = TILES * LANES
MESSAGE = (FRAME + 1) // 2 * LANES
VMEM_LIMIT = 40 * 1024 * 1024
BLOCK = 32
MESH = pl.DeviceIdType.MESH


def frame_slot(degree, order):
    if order == 0:
        return degree
    if order == 1:
        return 6 + degree
    if order == -1:
        return 12 + degree
    if order == 2:
        return 17 + degree
    return 22 + degree


def terms():
    listing = []
    spot = 0
    for degree in range(7):
        reach = min(degree, 2)
        span = 2 * degree + 1
        first = degree * degree
        for row in range(2 * reach + 1):
            slot = frame_slot(degree, row - reach)
            for tile in range(first // 2, (first + span - 1) // 2 + 1):
                ends = []
                for coeff in (2 * tile, 2 * tile + 1):
                    inside = first <= coeff < first + span
                    ends.append(spot + row * span + coeff - first if inside else None)
                listing.append((slot, tile, ends[0], ends[1]))
        spot += span * (2 * reach + 1)
    return listing


TERMS = terms()


def message_place(slot):
    return slot // 2, slot % 2


def far_first(count):
    return sorted(range(1, count), key=lambda offset: -min(offset, count - offset))


def cube_bits(count):
    bits = [1 << place for place in range(count.bit_length() - 1)]
    return bits if count == 1 << len(bits) else []


def each_peer(count, func):
    if count <= 17:
        for offset in far_first(count):
            func(offset - 1)
    else:
        each(count - 1, func)


def each(count, func):
    if count <= 16:
        for index in range(count):
            func(index)
    else:
        lax.fori_loop(0, count, lambda index, carry: (func(index), carry)[1], 0)


def kernel(
    peers,
    slots,
    x_hbm,
    rot_hbm,
    src_hbm,
    cnt_hbm,
    dst_hbm,
    gain_hbm,
    w0_hbm,
    w1_hbm,
    w2_hbm,
    out_ref,
    x_ref,
    rot_ref,
    src_ref,
    cnt_ref,
    dst_ref,
    gain_ref,
    w0,
    w1,
    w2,
    low_scr,
    high_scr,
    xg,
    own,
    packed,
    other,
    lhs,
    y_scr,
    msg,
    recv,
    rrot,
    mult,
    f_scr,
    back,
    total,
    sq,
    sq_other,
    wsem,
    esem,
    rot_send,
    rot_recv,
    msg_send,
    msg_recv,
    qsem,
    ready,
):
    me = lax.axis_index("dev")
    half = lax.axis_index("rep")
    nodes = x_ref.shape[0]
    flat = x_ref.shape[1]
    blocks = peers * slots // BLOCK
    group = BLOCK // slots
    partner = {"rep": 1 - half}

    def peer(offset):
        return lax.rem(me + offset, peers)

    loads = [
        pltpu.make_async_copy(src, dst, wsem.at[index])
        for index, (src, dst) in enumerate(
            (
                (x_hbm, x_ref),
                (rot_hbm, rot_ref),
                (src_hbm, src_ref),
                (cnt_hbm, cnt_ref),
                (dst_hbm, dst_ref),
                (gain_hbm, gain_ref),
                (w0_hbm, w0),
                (w1_hbm, w1),
                (w2_hbm, w2),
            )
        )
    ]
    for copy in loads:
        copy.start()
    barrier = pltpu.get_barrier_semaphore()
    pl.semaphore_signal(barrier, inc=1, device_id=partner, device_id_type=MESH)
    bits = cube_bits(peers)

    def across(bit):
        return me + bit - 2 * bit * lax.rem(me // bit, 2)

    for bit in bits:
        pl.semaphore_signal(barrier, inc=1, device_id={"dev": across(bit)}, device_id_type=MESH)
    if not bits:
        each(
            peers - 1,
            lambda o: pl.semaphore_signal(
                barrier, inc=1, device_id={"dev": peer(o + 1)}, device_id_type=MESH
            ),
        )

    lane = lax.broadcasted_iota(jnp.int32, (BLOCK, LANES), 1)
    low_half = lane < HALF
    mine = (lane // HALF) == half

    y_scr[...] = jnp.zeros_like(y_scr)
    xg[:, (TILES - 1) * LANES :] = jnp.zeros((BLOCK, LANES), jnp.float32)
    low_scr[...] = jnp.zeros_like(low_scr)
    high_scr[...] = jnp.zeros_like(high_scr)

    def column(rows):
        row = lax.broadcasted_iota(jnp.int32, (BLOCK, group), 0)
        spot = lax.broadcasted_iota(jnp.int32, (BLOCK, group), 1)
        chosen = jnp.zeros((BLOCK, group), jnp.float32)
        for index in range(slots):
            chosen = jnp.where(row == spot * slots + index, rows[index], chosen)
        return jnp.sum(chosen, axis=1, keepdims=True)

    def sources(block):
        count = cnt_ref[block]
        value = src_ref[block]
        return column(
            [
                jnp.where(count > index, value[index : index + 1], -1).astype(jnp.float32)
                for index in range(slots)
            ]
        )

    def targets(block):
        value = dst_ref[block].astype(jnp.float32)
        down = column([value[index : index + 1] for index in range(slots)])
        row = lax.broadcasted_iota(jnp.int32, (BLOCK, BLOCK), 0)
        spot = lax.broadcasted_iota(jnp.int32, (BLOCK, BLOCK), 1)
        return jnp.sum(jnp.where(row == spot, down, 0.0), axis=0, keepdims=True)

    def load_rotation(ref, start):
        for index in range(group):
            rows = ref[start + index].astype(jnp.float32)
            low_scr[index * slots : (index + 1) * slots, 0:WINDOW] = rows[:, 0:WINDOW]
            high_scr[index * slots : (index + 1) * slots, 0:WINDOW] = rows[:, ROT - WINDOW :]
        return low_scr[...], high_scr[...]

    def multiplier(tables, first, second):
        given = [entry for entry in (first, second) if entry is not None]
        which = 0 if max(given) < WINDOW else 1
        shift = which * (ROT - WINDOW)
        places = [WINDOW if e is None else e - shift for e in (first, second)]
        index = jnp.where(low_half, places[0], places[1])
        return jnp.take_along_axis(tables[which], index, axis=1, mode="promise_in_bounds")

    def turn(block):
        tables = load_rotation(rot_ref, block * group)
        hot = (
            lax.broadcasted_iota(jnp.int32, (BLOCK, nodes), 1).astype(jnp.float32) == sources(block)
        ).astype(jnp.bfloat16)
        xg[:, 0:flat] = jnp.dot(hot, x_ref[...], preferred_element_type=jnp.float32)
        sums = [None] * FRAME
        for slot, tile, first, second in TERMS:
            part = multiplier(tables, first, second) * xg[:, tile * LANES : (tile + 1) * LANES]
            sums[slot] = part if sums[slot] is None else sums[slot] + part
        for slot in range(FRAME):
            sums[slot] = sums[slot] + pltpu.roll(sums[slot], HALF, 1)
            own[block, :, slot * LANES : (slot + 1) * LANES] = sums[slot]
        for pair in range((FRAME + 1) // 2):
            first = sums[2 * pair]
            second = sums[min(2 * pair + 1, FRAME - 1)]
            packed[block, :, pair * LANES : (pair + 1) * LANES] = jnp.where(
                mine, first, second
            ).astype(jnp.bfloat16)

    for copy in loads[:4]:
        copy.wait()
    each(blocks, turn)

    pl.semaphore_wait(barrier, 1 + len(bits) if bits else peers)

    exchange = pltpu.make_async_remote_copy(
        src_ref=packed,
        dst_ref=other,
        send_sem=esem.at[0],
        recv_sem=esem.at[1],
        device_id=partner,
        device_id_type=MESH,
    )
    exchange.start()

    stages = bits[:-1]

    def tell(stage):
        if stage < len(stages):
            pl.semaphore_signal(
                ready.at[stage],
                inc=1,
                device_id={"dev": across(stages[stage])},
                device_id_type=MESH,
            )

    tell(0)
    for stage in range(len(stages) - 1):
        pl.semaphore_wait(ready.at[stage], 1)
        tell(stage + 1)

    def transfer(source, target, send, receive, o, landing):
        to = peer(o + 1)
        spot = me if landing is None else landing
        return pltpu.make_async_remote_copy(
            src_ref=source.at[to],
            dst_ref=target.at[spot],
            send_sem=send.at[to],
            recv_sem=receive.at[spot],
            device_id={"dev": to},
            device_id_type=MESH,
        )

    def rotations(o, landing=None):
        return transfer(rot_ref, rrot, rot_send, rot_recv, o, landing)

    def messages(o, landing=None):
        return transfer(msg, recv, msg_send, msg_recv, o, landing)

    for copy in loads[4:]:
        copy.wait()
    exchange.wait()

    def mix(block):
        for pair in range((FRAME + 1) // 2):
            there = other[block, :, pair * LANES : (pair + 1) * LANES].astype(jnp.float32)
            for slot, value in ((2 * pair, there), (2 * pair + 1, None)):
                if slot < FRAME:
                    value = pltpu.roll(there, HALF, 1) if value is None else value
                    cols = slice(slot * LANES, (slot + 1) * LANES)
                    lhs[:, cols] = jnp.where(mine, own[block, :, cols], value).astype(jnp.bfloat16)
        nt = (((1,), (1,)), ((), ()))
        y_scr[:, 0 : 7 * HALF] = lax.dot_general(
            lhs[:, 0 : 7 * LANES], w0[...], nt, preferred_element_type=jnp.float32
        )
        for start, count, ref, dims in (
            (7, 6, w1, (((1,), (0,)), ((), ()))),
            (19, 5, w2, nt),
        ):
            rows = jnp.concatenate(
                [
                    lhs[:, start * LANES : (start + count) * LANES],
                    lhs[:, (start + count) * LANES : (start + 2 * count) * LANES],
                ],
                axis=0,
            )
            real = lax.dot_general(rows, ref[0], dims, preferred_element_type=jnp.float32)
            imag = lax.dot_general(rows, ref[1], dims, preferred_element_type=jnp.float32)
            width = count * HALF
            plus = start * HALF
            minus = plus + width
            y_scr[:, plus : plus + width] = real[:BLOCK] - imag[BLOCK:]
            y_scr[:, minus : minus + width] = imag[:BLOCK] + real[BLOCK:]
        for index in range(group):
            msg[block * group + index] = y_scr[index * slots : (index + 1) * slots, :].astype(
                jnp.bfloat16
            )

    each(blocks, mix)
    if stages:
        pl.semaphore_wait(ready.at[len(stages) - 1], 1)
    each_peer(peers, lambda o: rotations(o).start())
    each_peer(peers, lambda o: messages(o).start())
    rrot[me] = rot_ref[me]
    recv[me] = msg[me]

    def wait_rotation(o):
        rotations(o, peer(o + 1)).wait_recv()

    def wait_message(o):
        messages(o, peer(o + 1)).wait_recv()

    each(peers - 1, wait_rotation)

    def prepare(block):
        tables = load_rotation(rrot, block * group)
        for number, (slot, tile, first, second) in enumerate(TERMS):
            mult[number] = multiplier(tables, first, second)

    def collect(block, add):
        for index in range(group):
            f_scr[index * slots : (index + 1) * slots, :] = recv[block * group + index].astype(
                jnp.float32
            )
        doubled = {}
        for slot in range(FRAME):
            tile, side = message_place(slot)
            value = f_scr[:, tile * LANES : (tile + 1) * LANES]
            turned = pltpu.roll(value, HALF, 1)
            doubled[slot] = (
                jnp.where(low_half, value, turned) if side == 0 else jnp.where(low_half, turned, value)
            )
        sums = [None] * TILES
        for number, (slot, tile, first, second) in enumerate(TERMS):
            part = mult[number] * doubled[slot]
            sums[tile] = part if sums[tile] is None else sums[tile] + part
        for tile in range(TILES):
            back[:, tile * LANES : (tile + 1) * LANES] = sums[tile].astype(jnp.bfloat16)
        hot = (
            lax.broadcasted_iota(jnp.int32, (nodes, BLOCK), 0).astype(jnp.float32) == targets(block)
        ).astype(jnp.bfloat16)
        value = jnp.dot(hot, back[...], preferred_element_type=jnp.float32)
        total[...] = total[...] + value if add else value

    if blocks == 1:
        prepare(0)
        each(peers - 1, wait_message)
        collect(0, False)
    else:
        each(peers - 1, wait_message)
        total[...] = jnp.zeros_like(total)

        def one(block, carry):
            prepare(block)
            collect(block, True)
            return carry

        lax.fori_loop(0, blocks, one, 0)

    partial = None
    for tile in range(TILES):
        value = total[:, tile * LANES : (tile + 1) * LANES]
        partial = value * value if partial is None else partial + value * value
    sq[...] = partial
    share = pltpu.make_async_remote_copy(
        src_ref=sq,
        dst_ref=sq_other,
        send_sem=qsem.at[0],
        recv_sem=qsem.at[1],
        device_id=partner,
        device_id_type=MESH,
    )
    share.start()
    each(peers - 1, lambda o: rotations(o).wait_send())
    each(peers - 1, lambda o: messages(o).wait_send())
    share.wait()
    mean_sq = jnp.sum(sq[...] + sq_other[...], axis=1, keepdims=True) / (2 * flat)
    scale = lax.rsqrt(mean_sq + 1e-06)
    for start in range(0, flat, LANES):
        cols = slice(start, min(start + LANES, flat))
        normed = total[:, cols] * scale
        out_ref[:, cols] = (
            x_ref[:, cols].astype(jnp.float32) + gain_ref[:, cols] * normed
        ).astype(jnp.bfloat16)


def shards(node_features, src_node, dst_node, counts, rotation, w_zero, w_one, w_two, norm_gain):
    nodes, _, flat = node_features.shape
    peers, slots = src_node.shape[1:]
    edges = peers * slots
    blocks = edges // BLOCK
    x = node_features.reshape(nodes, flat)
    group = peers // blocks
    src = src_node.reshape(blocks, group, slots).swapaxes(1, 2)
    dst = dst_node.reshape(blocks, group, slots).swapaxes(1, 2)
    cnt = counts.reshape(blocks, 1, group)
    rot = rotation.reshape(peers, slots, ROT)
    w0 = w_zero.reshape(w_zero.shape[0], -1).T
    w1 = w_one.reshape(2, w_one.shape[1], -1)
    w2 = w_two.reshape(2, w_two.shape[1], -1).swapaxes(1, 2)
    vmem = pl.BlockSpec(memory_space=pltpu.VMEM)
    hbm = pl.BlockSpec(memory_space=pltpu.HBM)
    f32, bf16 = jnp.float32, jnp.bfloat16
    dma = pltpu.SemaphoreType.DMA
    pairs = (FRAME + 1) // 2
    operands = (x, rot, src, cnt, dst, norm_gain, w0, w1, w2)
    out = pl.pallas_call(
        functools.partial(kernel, peers, slots),
        out_shape=jax.ShapeDtypeStruct((nodes, flat), bf16),
        in_specs=[hbm] * 9,
        out_specs=vmem,
        scratch_shapes=[
            pltpu.VMEM(x.shape, bf16),
            pltpu.VMEM(rot.shape, bf16),
            pltpu.VMEM(src.shape, jnp.int32),
            pltpu.VMEM(cnt.shape, jnp.int32),
            pltpu.VMEM(dst.shape, jnp.int32),
            pltpu.VMEM(norm_gain.shape, f32),
            pltpu.VMEM(w0.shape, bf16),
            pltpu.VMEM(w1.shape, bf16),
            pltpu.VMEM(w2.shape, bf16),
            pltpu.VMEM((BLOCK, LANES), f32),
            pltpu.VMEM((BLOCK, LANES), f32),
            pltpu.VMEM((BLOCK, WIDE), f32),
            pltpu.VMEM((blocks, BLOCK, FRAME * LANES), f32),
            pltpu.VMEM((blocks, BLOCK, pairs * LANES), bf16),
            pltpu.VMEM((blocks, BLOCK, pairs * LANES), bf16),
            pltpu.VMEM((BLOCK, FRAME * LANES), bf16),
            pltpu.VMEM((BLOCK, MESSAGE), f32),
            pltpu.VMEM((peers, slots, MESSAGE), bf16),
            pltpu.VMEM((peers, slots, MESSAGE), bf16),
            pltpu.VMEM((peers, slots, ROT), bf16),
            pltpu.VMEM((len(TERMS), BLOCK, LANES), f32),
            pltpu.VMEM((BLOCK, MESSAGE), f32),
            pltpu.VMEM((BLOCK, WIDE), bf16),
            pltpu.VMEM((nodes, WIDE), f32),
            pltpu.VMEM((nodes, LANES), f32),
            pltpu.VMEM((nodes, LANES), f32),
            dma((9,)),
            dma((2,)),
            dma((peers,)),
            dma((peers,)),
            dma((peers,)),
            dma((peers,)),
            dma((2,)),
            pltpu.SemaphoreType.REGULAR((max(1, len(cube_bits(peers))),)),
        ],
        compiler_params=pltpu.CompilerParams(
            collective_id=0, has_side_effects=True, vmem_limit_bytes=VMEM_LIMIT
        ),
    )(*(pltpu.with_memory_space_constraint(operand, pltpu.HBM) for operand in operands))
    return out.reshape(nodes, 1, flat)


def solution(mesh):
    return jax.shard_map(
        shards,
        mesh=mesh,
        in_specs=(
            P("dev", "rep", None),
            P("dev", None, None),
            P("dev", None, None),
            P("dev", None),
            P("dev", None, None, None),
            P(None, "rep", None),
            P(None, None, "rep", None),
            P(None, None, "rep", None),
            P("rep", None),
        ),
        out_specs=P("dev", "rep", None),
        check_vma=False,
    )
```

```python
import functools

import jax
import jax.numpy as jnp
from jax import lax
from jax.experimental import pallas as pl
from jax.experimental.pallas import tpu as pltpu
from jax.sharding import PartitionSpec as P

LANES = 128
HALF = 64
COEFFS = 49
FRAME = 29
CUT = 20
ROT = 235
WINDOW = 120
TILES = (COEFFS + 1) // 2
WIDE = TILES * LANES
MESSAGE = (FRAME + 1) // 2 * LANES
VMEM_LIMIT = 40 * 1024 * 1024
BLOCK = 32
MESH = pl.DeviceIdType.MESH


def frame_slot(degree, order):
    if order == 0:
        return degree
    if order == 1:
        return 6 + degree
    if order == -1:
        return 12 + degree
    if order == 2:
        return 17 + degree
    return 22 + degree


def terms():
    listing = []
    spot = 0
    for degree in range(7):
        reach = min(degree, 2)
        span = 2 * degree + 1
        first = degree * degree
        for row in range(2 * reach + 1):
            slot = frame_slot(degree, row - reach)
            for tile in range(first // 2, (first + span - 1) // 2 + 1):
                ends = []
                for coeff in (2 * tile, 2 * tile + 1):
                    inside = first <= coeff < first + span
                    ends.append(spot + row * span + coeff - first if inside else None)
                listing.append((slot, tile, ends[0], ends[1]))
        spot += span * (2 * reach + 1)
    return listing


TERMS = terms()


def message_place(slot):
    return slot // 2, slot % 2


def far_first(count):
    return sorted(range(1, count), key=lambda offset: -min(offset, count - offset))


def each_peer(count, func):
    if count <= 17:
        for offset in far_first(count):
            func(offset - 1)
    else:
        each(count - 1, func)


def each(count, func):
    if count <= 16:
        for index in range(count):
            func(index)
    else:
        lax.fori_loop(0, count, lambda index, carry: (func(index), carry)[1], 0)


def kernel(
    peers,
    slots,
    x_hbm,
    rot_hbm,
    src_hbm,
    cnt_hbm,
    dst_hbm,
    gain_hbm,
    w0_hbm,
    w1_hbm,
    w2_hbm,
    out_ref,
    x_ref,
    rot_ref,
    src_ref,
    cnt_ref,
    dst_ref,
    gain_ref,
    w0,
    w1,
    w2,
    low_scr,
    high_scr,
    xg,
    own,
    packed,
    other,
    lhs,
    y_scr,
    msg,
    recv,
    rrot,
    mult,
    f_scr,
    back,
    total,
    sq,
    sq_other,
    wsem,
    esem,
    rot_send,
    rot_recv,
    msg_send,
    msg_recv,
    qsem,
):
    me = lax.axis_index("dev")
    half = lax.axis_index("rep")
    nodes = x_ref.shape[0]
    flat = x_ref.shape[1]
    blocks = peers * slots // BLOCK
    group = BLOCK // slots
    partner = {"rep": 1 - half}

    def peer(offset):
        return lax.rem(me + offset, peers)

    loads = [
        pltpu.make_async_copy(src, dst, wsem.at[index])
        for index, (src, dst) in enumerate(
            (
                (x_hbm, x_ref),
                (rot_hbm, rot_ref),
                (src_hbm, src_ref),
                (cnt_hbm, cnt_ref),
                (dst_hbm, dst_ref),
                (gain_hbm, gain_ref),
                (w0_hbm, w0),
                (w1_hbm, w1),
                (w2_hbm, w2),
            )
        )
    ]
    for copy in loads:
        copy.start()
    barrier = pltpu.get_barrier_semaphore()
    pl.semaphore_signal(barrier, inc=1, device_id=partner, device_id_type=MESH)
    each(
        peers - 1,
        lambda o: pl.semaphore_signal(
            barrier, inc=1, device_id={"dev": peer(o + 1)}, device_id_type=MESH
        ),
    )

    lane = lax.broadcasted_iota(jnp.int32, (BLOCK, LANES), 1)
    low_half = lane < HALF
    mine = (lane // HALF) == half

    y_scr[...] = jnp.zeros_like(y_scr)
    xg[:, (TILES - 1) * LANES :] = jnp.zeros((BLOCK, LANES), jnp.float32)
    low_scr[...] = jnp.zeros_like(low_scr)
    high_scr[...] = jnp.zeros_like(high_scr)

    def column(rows):
        row = lax.broadcasted_iota(jnp.int32, (BLOCK, group), 0)
        spot = lax.broadcasted_iota(jnp.int32, (BLOCK, group), 1)
        chosen = jnp.zeros((BLOCK, group), jnp.float32)
        for index in range(slots):
            chosen = jnp.where(row == spot * slots + index, rows[index], chosen)
        return jnp.sum(chosen, axis=1, keepdims=True)

    def sources(block):
        count = cnt_ref[block]
        value = src_ref[block]
        return column(
            [
                jnp.where(count > index, value[index : index + 1], -1).astype(jnp.float32)
                for index in range(slots)
            ]
        )

    def targets(block):
        value = dst_ref[block].astype(jnp.float32)
        down = column([value[index : index + 1] for index in range(slots)])
        row = lax.broadcasted_iota(jnp.int32, (BLOCK, BLOCK), 0)
        spot = lax.broadcasted_iota(jnp.int32, (BLOCK, BLOCK), 1)
        return jnp.sum(jnp.where(row == spot, down, 0.0), axis=0, keepdims=True)

    def load_rotation(ref, start):
        for index in range(group):
            rows = ref[start + index].astype(jnp.float32)
            low_scr[index * slots : (index + 1) * slots, 0:WINDOW] = rows[:, 0:WINDOW]
            high_scr[index * slots : (index + 1) * slots, 0:WINDOW] = rows[:, ROT - WINDOW :]
        return low_scr[...], high_scr[...]

    def multiplier(tables, first, second):
        given = [entry for entry in (first, second) if entry is not None]
        which = 0 if max(given) < WINDOW else 1
        shift = which * (ROT - WINDOW)
        places = [WINDOW if e is None else e - shift for e in (first, second)]
        index = jnp.where(low_half, places[0], places[1])
        return jnp.take_along_axis(tables[which], index, axis=1, mode="promise_in_bounds")

    middle = CUT // 2 * LANES
    exchanges = [
        pltpu.make_async_remote_copy(
            src_ref=packed.at[:, :, cols],
            dst_ref=other.at[:, :, cols],
            send_sem=esem.at[2 * index],
            recv_sem=esem.at[2 * index + 1],
            device_id=partner,
            device_id_type=MESH,
        )
        for index, cols in enumerate(
            (pl.ds(0, middle), pl.ds(middle, (FRAME + 1) // 2 * LANES - middle))
        )
    ]

    def turn(block):
        tables = load_rotation(rot_ref, block * group)
        hot = (
            lax.broadcasted_iota(jnp.int32, (BLOCK, nodes), 1).astype(jnp.float32) == sources(block)
        ).astype(jnp.bfloat16)
        xg[:, 0:flat] = jnp.dot(hot, x_ref[...], preferred_element_type=jnp.float32)
        rotate(block, tables, 0, CUT)
        if blocks == 1:
            pl.semaphore_wait(barrier, peers)
            exchanges[0].start()
        rotate(block, tables, CUT, FRAME)

    def rotate(block, tables, begin, end):
        sums = [None] * FRAME
        for slot, tile, first, second in TERMS:
            if not begin <= slot < end:
                continue
            part = multiplier(tables, first, second) * xg[:, tile * LANES : (tile + 1) * LANES]
            sums[slot] = part if sums[slot] is None else sums[slot] + part
        for slot in range(begin, end):
            sums[slot] = sums[slot] + pltpu.roll(sums[slot], HALF, 1)
            own[block, :, slot * LANES : (slot + 1) * LANES] = sums[slot]
        for pair in range(begin // 2, (end + 1) // 2):
            first = sums[2 * pair]
            second = sums[min(2 * pair + 1, FRAME - 1)]
            packed[block, :, pair * LANES : (pair + 1) * LANES] = jnp.where(
                mine, first, second
            ).astype(jnp.bfloat16)

    for copy in loads[:4]:
        copy.wait()
    each(blocks, turn)

    if blocks > 1:
        pl.semaphore_wait(barrier, peers)
        exchanges[0].start()
    exchanges[1].start()

    def transfer(source, target, send, receive, o, landing):
        to = peer(o + 1)
        spot = me if landing is None else landing
        return pltpu.make_async_remote_copy(
            src_ref=source.at[to],
            dst_ref=target.at[spot],
            send_sem=send.at[to],
            recv_sem=receive.at[spot],
            device_id={"dev": to},
            device_id_type=MESH,
        )

    def rotations(o, landing=None):
        return transfer(rot_ref, rrot, rot_send, rot_recv, o, landing)

    def messages(o, landing=None):
        return transfer(msg, recv, msg_send, msg_recv, o, landing)

    each_peer(peers, lambda o: rotations(o).start())
    rrot[me] = rot_ref[me]

    for copy in loads[4:]:
        copy.wait()
    for copy in exchanges:
        copy.wait()

    def mix(block):
        for pair in range((FRAME + 1) // 2):
            there = other[block, :, pair * LANES : (pair + 1) * LANES].astype(jnp.float32)
            for slot, value in ((2 * pair, there), (2 * pair + 1, None)):
                if slot < FRAME:
                    value = pltpu.roll(there, HALF, 1) if value is None else value
                    cols = slice(slot * LANES, (slot + 1) * LANES)
                    lhs[:, cols] = jnp.where(mine, own[block, :, cols], value).astype(jnp.bfloat16)
        nt = (((1,), (1,)), ((), ()))
        y_scr[:, 0 : 7 * HALF] = lax.dot_general(
            lhs[:, 0 : 7 * LANES], w0[...], nt, preferred_element_type=jnp.float32
        )
        for start, count, ref, dims in (
            (7, 6, w1, (((1,), (0,)), ((), ()))),
            (19, 5, w2, nt),
        ):
            rows = jnp.concatenate(
                [
                    lhs[:, start * LANES : (start + count) * LANES],
                    lhs[:, (start + count) * LANES : (start + 2 * count) * LANES],
                ],
                axis=0,
            )
            real = lax.dot_general(rows, ref[0], dims, preferred_element_type=jnp.float32)
            imag = lax.dot_general(rows, ref[1], dims, preferred_element_type=jnp.float32)
            width = count * HALF
            plus = start * HALF
            minus = plus + width
            y_scr[:, plus : plus + width] = real[:BLOCK] - imag[BLOCK:]
            y_scr[:, minus : minus + width] = imag[:BLOCK] + real[BLOCK:]
        for index in range(group):
            msg[block * group + index] = y_scr[index * slots : (index + 1) * slots, :].astype(
                jnp.bfloat16
            )

    each(blocks, mix)
    each_peer(peers, lambda o: messages(o).start())
    recv[me] = msg[me]

    def wait_rotation(o):
        rotations(o, peer(o + 1)).wait_recv()

    def wait_message(o):
        messages(o, peer(o + 1)).wait_recv()

    each(peers - 1, wait_rotation)

    def prepare(block):
        tables = load_rotation(rrot, block * group)
        for number, (slot, tile, first, second) in enumerate(TERMS):
            mult[number] = multiplier(tables, first, second)

    def collect(block, add):
        for index in range(group):
            f_scr[index * slots : (index + 1) * slots, :] = recv[block * group + index].astype(
                jnp.float32
            )
        doubled = {}
        for slot in range(FRAME):
            tile, side = message_place(slot)
            value = f_scr[:, tile * LANES : (tile + 1) * LANES]
            turned = pltpu.roll(value, HALF, 1)
            doubled[slot] = (
                jnp.where(low_half, value, turned) if side == 0 else jnp.where(low_half, turned, value)
            )
        sums = [None] * TILES
        for number, (slot, tile, first, second) in enumerate(TERMS):
            part = mult[number] * doubled[slot]
            sums[tile] = part if sums[tile] is None else sums[tile] + part
        for tile in range(TILES):
            back[:, tile * LANES : (tile + 1) * LANES] = sums[tile].astype(jnp.bfloat16)
        hot = (
            lax.broadcasted_iota(jnp.int32, (nodes, BLOCK), 0).astype(jnp.float32) == targets(block)
        ).astype(jnp.bfloat16)
        value = jnp.dot(hot, back[...], preferred_element_type=jnp.float32)
        total[...] = total[...] + value if add else value

    if blocks == 1:
        prepare(0)
        each(peers - 1, wait_message)
        collect(0, False)
    else:
        each(peers - 1, wait_message)
        total[...] = jnp.zeros_like(total)

        def one(block, carry):
            prepare(block)
            collect(block, True)
            return carry

        lax.fori_loop(0, blocks, one, 0)

    partial = None
    for tile in range(TILES):
        value = total[:, tile * LANES : (tile + 1) * LANES]
        partial = value * value if partial is None else partial + value * value
    sq[...] = partial
    share = pltpu.make_async_remote_copy(
        src_ref=sq,
        dst_ref=sq_other,
        send_sem=qsem.at[0],
        recv_sem=qsem.at[1],
        device_id=partner,
        device_id_type=MESH,
    )
    share.start()
    each(peers - 1, lambda o: rotations(o).wait_send())
    each(peers - 1, lambda o: messages(o).wait_send())
    share.wait()
    mean_sq = jnp.sum(sq[...] + sq_other[...], axis=1, keepdims=True) / (2 * flat)
    scale = lax.rsqrt(mean_sq + 1e-06)
    for start in range(0, flat, LANES):
        cols = slice(start, min(start + LANES, flat))
        normed = total[:, cols] * scale
        out_ref[:, cols] = (
            x_ref[:, cols].astype(jnp.float32) + gain_ref[:, cols] * normed
        ).astype(jnp.bfloat16)


def shards(node_features, src_node, dst_node, counts, rotation, w_zero, w_one, w_two, norm_gain):
    nodes, _, flat = node_features.shape
    peers, slots = src_node.shape[1:]
    edges = peers * slots
    blocks = edges // BLOCK
    x = node_features.reshape(nodes, flat)
    group = peers // blocks
    src = src_node.reshape(blocks, group, slots).swapaxes(1, 2)
    dst = dst_node.reshape(blocks, group, slots).swapaxes(1, 2)
    cnt = counts.reshape(blocks, 1, group)
    rot = rotation.reshape(peers, slots, ROT)
    w0 = w_zero.reshape(w_zero.shape[0], -1).T
    w1 = w_one.reshape(2, w_one.shape[1], -1)
    w2 = w_two.reshape(2, w_two.shape[1], -1).swapaxes(1, 2)
    vmem = pl.BlockSpec(memory_space=pltpu.VMEM)
    hbm = pl.BlockSpec(memory_space=pltpu.HBM)
    f32, bf16 = jnp.float32, jnp.bfloat16
    dma = pltpu.SemaphoreType.DMA
    pairs = (FRAME + 1) // 2
    operands = (x, rot, src, cnt, dst, norm_gain, w0, w1, w2)
    out = pl.pallas_call(
        functools.partial(kernel, peers, slots),
        out_shape=jax.ShapeDtypeStruct((nodes, flat), bf16),
        in_specs=[hbm] * 9,
        out_specs=vmem,
        scratch_shapes=[
            pltpu.VMEM(x.shape, bf16),
            pltpu.VMEM(rot.shape, bf16),
            pltpu.VMEM(src.shape, jnp.int32),
            pltpu.VMEM(cnt.shape, jnp.int32),
            pltpu.VMEM(dst.shape, jnp.int32),
            pltpu.VMEM(norm_gain.shape, f32),
            pltpu.VMEM(w0.shape, bf16),
            pltpu.VMEM(w1.shape, bf16),
            pltpu.VMEM(w2.shape, bf16),
            pltpu.VMEM((BLOCK, LANES), f32),
            pltpu.VMEM((BLOCK, LANES), f32),
            pltpu.VMEM((BLOCK, WIDE), f32),
            pltpu.VMEM((blocks, BLOCK, FRAME * LANES), f32),
            pltpu.VMEM((blocks, BLOCK, pairs * LANES), bf16),
            pltpu.VMEM((blocks, BLOCK, pairs * LANES), bf16),
            pltpu.VMEM((BLOCK, FRAME * LANES), bf16),
            pltpu.VMEM((BLOCK, MESSAGE), f32),
            pltpu.VMEM((peers, slots, MESSAGE), bf16),
            pltpu.VMEM((peers, slots, MESSAGE), bf16),
            pltpu.VMEM((peers, slots, ROT), bf16),
            pltpu.VMEM((len(TERMS), BLOCK, LANES), f32),
            pltpu.VMEM((BLOCK, MESSAGE), f32),
            pltpu.VMEM((BLOCK, WIDE), bf16),
            pltpu.VMEM((nodes, WIDE), f32),
            pltpu.VMEM((nodes, LANES), f32),
            pltpu.VMEM((nodes, LANES), f32),
            dma((9,)),
            dma((4,)),
            dma((peers,)),
            dma((peers,)),
            dma((peers,)),
            dma((peers,)),
            dma((2,)),
        ],
        compiler_params=pltpu.CompilerParams(
            collective_id=0, has_side_effects=True, vmem_limit_bytes=VMEM_LIMIT
        ),
    )(*(pltpu.with_memory_space_constraint(operand, pltpu.HBM) for operand in operands))
    return out.reshape(nodes, 1, flat)


def solution(mesh):
    return jax.shard_map(
        shards,
        mesh=mesh,
        in_specs=(
            P("dev", "rep", None),
            P("dev", None, None),
            P("dev", None, None),
            P("dev", None),
            P("dev", None, None, None),
            P(None, "rep", None),
            P(None, None, "rep", None),
            P(None, None, "rep", None),
            P("rep", None),
        ),
        out_specs=P("dev", "rep", None),
        check_vma=False,
    )
```
